32 devices in a mesh: cell: 16 (over z, y, x), gene: 2 (over core).
Axes of the slice: x: 2, y: 2, z: 4, core: 2. Of those that a mesh axis runs over, the one named last changes fastest.
Arguments:
- tiles: bfloat16 [2, 1024, 128, 128], P('gene', 'cell'), may hold values from -8 to 8
- tile_row: int32 [2, 1024], P('gene', 'cell'), may hold values from 0 to 7, as said below
- tile_col: int32 [2, 1024], P('gene', 'cell'), may hold values from 0 to 15
- tile_count: int32 [2, 16], P('gene', 'cell'), may hold values from 1 to 64, as said below
- start_basis: bfloat16 [64, 4096], P(None, 'gene'), may hold values from -0.09375 to 0.09375
Outputs:
- basis: bfloat16 [64, 16384], P(None, 'cell')
- loadings: float32 [64, 4096], P(None, ('gene', 'cell'))
The draws below stay inside these ranges and needn't reach their ends.
Inputs may be any that keep to these rules, and one draw needn't show every extreme that they name: `tile_row`: tile row of each slot, within 0 to 7; the slots of one device name distinct (row, column) pairs. `tile_count`: slots in use; for each index of gene some device uses all 64.
All inputs are finite; a program needn't handle non-finite values.
Results may differ from the reference program's by a relative error of at most 0.018.
Values may be sent and summed in bfloat16 or wider, within the bound.
No kernel may reach another device: no remote copies, remote signals or barrier semaphores. Data moves between devices by JAX's collectives and lax.ppermute only.
A program may use at most 64 MiB of HBM per device.

```python
import jax
import jax.numpy as jnp
from jax import lax

K = 64
G = 4096
TILE = 128
ROW_BLOCKS = 8
N_CELL = 16
N_GENE = 2


strongest = 32.0


tile_scale = 0.125


def slot_places(key):
    base = jax.random.fold_in(key, 7)
    gene_blocks = G // (N_GENE * TILE)
    slot_count = ROW_BLOCKS * gene_blocks // 2
    keys = jax.random.split(base, N_GENE * N_CELL)

    def one_device(device_key):
        return jax.random.permutation(device_key, ROW_BLOCKS * gene_blocks)[:slot_count].astype(jnp.int32)
    places = jax.vmap(one_device)(keys)
    return (places.reshape(N_GENE, N_CELL * slot_count), gene_blocks)


def draw_tiles(key, part):
    places, gene_blocks = slot_places(key)
    slot_count = ROW_BLOCKS * gene_blocks // 2
    columns_all = G // TILE
    per_column = (K + columns_all - 1) // columns_all
    row_local = places // gene_blocks
    col_local = places % gene_blocks
    gene_of = jnp.arange(N_GENE, dtype=jnp.int32)[:, None]
    cell_of = (jnp.arange(N_CELL * slot_count, dtype=jnp.int32) // slot_count)[None, :]
    global_col = (gene_of * gene_blocks + col_local).reshape(N_GENE * N_CELL, slot_count).astype(jnp.int32)
    global_row = (cell_of * ROW_BLOCKS + row_local).reshape(N_GENE * N_CELL, slot_count).astype(jnp.int32)
    ladder = strongest ** (jnp.arange(K, dtype=jnp.float32) / jnp.float32(K - 1))
    order = jax.random.permutation(jax.random.fold_in(key, 21), K)
    strength = ladder[order]
    component = jnp.arange(columns_all, dtype=jnp.int32)[:, None] + columns_all * jnp.arange(per_column, dtype=jnp.int32)[None, :]
    column_strength = jnp.where(component < K, strength[jnp.minimum(component, K - 1)], 0.0)
    gene_factor = jax.random.truncated_normal(jax.random.fold_in(key, 23), -3.0, 3.0, (columns_all, per_column, TILE), jnp.float32)
    gene_factor = gene_factor / jnp.sqrt(jnp.float32(TILE))
    cell_key = jax.random.fold_in(key, 27)
    noise_key = jax.random.fold_in(key, 25)
    rise_ratio = 3.0

    def one_device(index):
        columns = global_col[index]
        rows = global_row[index]
        cell_index = (index % N_CELL).astype(jnp.float32)
        rise = jnp.float32(rise_ratio) ** (cell_index / jnp.float32(max(N_CELL - 1, 1)))
        slot_keys = jax.vmap(lambda row, col: jax.random.fold_in(cell_key, row * columns_all + col))(rows, columns)
        device_key = jax.random.fold_in(noise_key, index)
        cell_factor = jax.vmap(lambda one_key: jax.random.truncated_normal(one_key, -3.0, 3.0, (per_column, TILE), jnp.float32))(slot_keys)
        noise = jax.random.truncated_normal(device_key, -4.0, 4.0, (slot_count, TILE, TILE), jnp.float32)
        weighted = cell_factor * column_strength[columns][:, :, None]
        planted = jnp.einsum('spr,spg->srg', weighted, gene_factor[columns])
        return jnp.clip(tile_scale * rise * (noise + planted), -8.0, 8.0).astype(jnp.bfloat16)
    stacked = lax.map(one_device, jnp.arange(N_GENE * N_CELL, dtype=jnp.int32))
    return stacked.reshape(N_GENE, N_CELL * slot_count, TILE, TILE)


def draw_tile_row(key, part):
    places, gene_blocks = slot_places(key)
    return (places // gene_blocks).astype(jnp.int32)


def draw_tile_col(key, part):
    places, gene_blocks = slot_places(key)
    return (places % gene_blocks).astype(jnp.int32)


def draw_tile_count(key, part):
    slot_count = ROW_BLOCKS * (G // (N_GENE * TILE)) // 2
    first_key, second_key = jax.random.split(jax.random.fold_in(key, 11))
    lowest = max(1, slot_count // 8)
    highest = max(lowest + 1, slot_count * 7 // 8 + 1)
    counts = jax.random.randint(first_key, (N_GENE, N_CELL), lowest, highest, dtype=jnp.int32)
    fullest = jax.random.randint(second_key, (N_GENE, 1), 0, N_CELL, dtype=jnp.int32)
    return jnp.where(jnp.arange(N_CELL, dtype=jnp.int32)[None, :] == fullest, slot_count, counts).astype(jnp.int32)


def block_scale(key, shape, pieces, least, high):
    gain = 1.0
    for dim, blocks in pieces:
        steps = jax.random.uniform(jax.random.fold_in(jax.random.fold_in(key, 6), dim), (blocks,), jnp.float32, least / len(pieces), high / len(pieces))
        gain = gain * jnp.repeat(jnp.exp(steps), shape[dim] // blocks).reshape((-1,) + (1,) * (len(shape) - 1 - dim))
    return gain


def scatter_about(key, extent, width, bound, cuts=(), kind=jnp.bfloat16):
    values = jax.random.normal(key, extent, jnp.float32) * width
    if len(cuts) > 0:
        values = block_scale(key, extent, cuts, -0.22, 0.18) * values
    return jnp.clip(values, min=-bound, max=bound).astype(kind)


def setup_inputs(seed: int = 0) -> dict:
    key_list = jax.random.split(jax.random.key(seed), 6)
    tiles = draw_tiles(jax.random.fold_in(key_list[5], 71), 0)
    tile_row = draw_tile_row(jax.random.fold_in(key_list[5], 71), 0)
    tile_col = draw_tile_col(jax.random.fold_in(key_list[5], 71), 0)
    tile_count = draw_tile_count(jax.random.fold_in(key_list[5], 71), 0)
    start_basis = scatter_about(key_list[4], (K, G), G ** -0.5, 0.09375, ((1, 2),))
    return {"tiles": tiles, "tile_row": tile_row, "tile_col": tile_col, "tile_count": tile_count, "start_basis": start_basis}


def solve_lower(lower, right):
    return lax.linalg.triangular_solve(lower, right, left_side=True, lower=True)

def gram_of(scores):
    return jnp.dot(scores.astype(jnp.float32), scores.T.astype(jnp.float32), precision=lax.Precision.HIGHEST, preferred_element_type=jnp.float32)

def orthonormal(scores):
    lower_one = jnp.linalg.cholesky(gram_of(scores))
    return solve_lower(lower_one, scores)

def reference(tiles, tile_row, tile_col, tile_count, start_basis):
    slot_count = tiles.shape[1] // N_CELL
    gene_dev = G // N_GENE
    gene_blocks = gene_dev // TILE
    cell_dev = ROW_BLOCKS * TILE
    grouped = tiles.reshape(N_GENE, N_CELL, slot_count, TILE, TILE)
    rows_all = tile_row.reshape(N_GENE, N_CELL, slot_count)
    cols_all = tile_col.reshape(N_GENE, N_CELL, slot_count)

    def onehots(gene, cell):
        live_mask = (jnp.arange(slot_count) < tile_count[gene, cell]).astype(jnp.float32)
        row_hot = (rows_all[gene, cell][:, None] == jnp.arange(ROW_BLOCKS)[None, :]).astype(jnp.float32) * live_mask[:, None]
        col_hot = (cols_all[gene, cell][:, None] == jnp.arange(gene_blocks)[None, :]).astype(jnp.float32) * live_mask[:, None]
        return (row_hot, col_hot)

    def scores_of(basis):

        def one_cell(cell):
            total = jnp.zeros((K, cell_dev), jnp.float32)
            for gene in range(N_GENE):
                row_hot, col_hot = onehots(gene, cell)
                local = basis[:, gene * gene_dev:(gene + 1) * gene_dev].reshape(K, gene_blocks, TILE)
                picked = jnp.take(local, cols_all[gene, cell], axis=1).astype(jnp.float32)
                products = jnp.einsum('ksg,srg->skr', picked, grouped[gene, cell].astype(jnp.float32), precision=lax.Precision.HIGHEST)
                summed = jnp.einsum('sb,skr->kbr', row_hot, products, precision=lax.Precision.HIGHEST)
                total = total + summed.reshape(K, cell_dev)
            return total
        stacked = lax.map(one_cell, jnp.arange(N_CELL))
        return jnp.transpose(stacked, (1, 0, 2)).reshape(K, N_CELL * cell_dev)

    def loadings_of(ortho_half):
        blocks = ortho_half.reshape(K, N_CELL, cell_dev)

        def step(carry, cell):
            parts = []
            for gene in range(N_GENE):
                row_hot, col_hot = onehots(gene, cell)
                local = blocks[:, cell].reshape(K, ROW_BLOCKS, TILE)
                picked = jnp.take(local, rows_all[gene, cell], axis=1).astype(jnp.float32)
                products = jnp.einsum('ksr,srg->skg', picked, grouped[gene, cell].astype(jnp.float32), precision=lax.Precision.HIGHEST)
                summed = jnp.einsum('sb,skg->kbg', col_hot, products, precision=lax.Precision.HIGHEST)
                parts.append(summed.reshape(K, gene_dev))
            return (carry + jnp.stack(parts), None)
        start = jnp.zeros((N_GENE, K, gene_dev), jnp.float32)
        total, _ = lax.scan(step, start, jnp.arange(N_CELL))
        return jnp.transpose(total, (1, 0, 2)).reshape(K, G)
    ortho = orthonormal(scores_of(start_basis))
    middle = loadings_of(ortho.astype(jnp.bfloat16))
    ortho_two = orthonormal(scores_of(middle.astype(jnp.bfloat16)))
    loadings = loadings_of(ortho_two.astype(jnp.bfloat16))
    basis = (ortho_two * jnp.sqrt(jnp.float32(N_CELL * cell_dev))).astype(jnp.bfloat16)
    return (basis, loadings)
```

```python
import functools

import jax
import jax.numpy as jnp
from jax import lax
from jax.experimental import pallas as pl
from jax.experimental.pallas import tpu as pltpu
from jax.sharding import PartitionSpec as P

ROW_BLOCKS = 8
BF = jnp.bfloat16
F32 = jnp.float32
HIGH = lax.Precision.HIGHEST
NT = (((1,), (1,)), ((), ()))
TN = (((0,), (0,)), ((), ()))
NN = (((1,), (0,)), ((), ()))
VMEM = pl.BlockSpec(memory_space=pltpu.VMEM)
SMEM = pl.BlockSpec(memory_space=pltpu.SMEM)
ANY = pl.BlockSpec(memory_space=pl.ANY)


def dot(a, b, dims, precision=None):
    return lax.dot_general(a, b, dims, precision=precision, preferred_element_type=F32)


def dense_kernel(row, col, count, tiles, basis, x_ref, s_ref, held, sems):
    tile = tiles.shape[-1]
    rows = x_ref.shape[0] // tile
    cols = x_ref.shape[1] // tile

    def place(r, c):
        return x_ref.at[pl.ds(pl.multiple_of(r * tile, tile), tile), pl.ds(pl.multiple_of(c * tile, tile), tile)]

    def copy(s):
        return pltpu.make_async_copy(tiles.at[s], place(row[0, s], col[0, s]), sems.at[s])

    for i in range(rows * cols):
        held[i] = 0
    live = count[0, 0]

    def start(s, _):
        copy(s).start()
        held[row[0, s] * cols + col[0, s]] = 1
        return 0

    lax.fori_loop(0, live, start, 0)

    def clear(i, _):
        @pl.when(held[i] == 0)
        def _():
            spot = place(i // cols, lax.rem(i, cols))
            spot[...] = jnp.zeros((tile, tile), BF)

        return 0

    lax.fori_loop(0, rows * cols, clear, 0)

    def finish(s, _):
        copy(s).wait()
        return 0

    lax.fori_loop(0, live, finish, 0)
    s_ref[...] = dot(basis[...], x_ref[...], NT)


def scores_kernel(pieces, x, s_ref):
    s_ref[...] = dot(pieces[...], x[...], NT)


def share_kernel(me, own, other, x, y_ref, gram_ref, total_ref=None):
    total = own[...] + other[...]
    if total_ref is not None:
        total_ref[...] = total
    k = total.shape[0]
    high = total.astype(BF)
    low = (total - high.astype(F32)).astype(BF)
    both = jnp.concatenate([high, low], axis=0)
    g = dot(both, high, NT)
    h = dot(both, low, NT)
    gram_ref[...] = (g[:k] + (g[k:] + h[:k])) + h[k:]
    y = dot(both, x[...], NN)
    y = y[:k] + y[k:]
    if len(y_ref.shape) == 2:
        y_ref[...] = y
    else:
        n, _, wide = y_ref.shape
        for q in range(n):
            y_ref[jnp.bitwise_xor(me[0], q)] = y[:, q * wide : (q + 1) * wide]


def lower_inverse(gram, block=8):
    k = gram.shape[0]
    eye = (lax.broadcasted_iota(jnp.int32, (k, k), 0) == lax.broadcasted_iota(jnp.int32, (k, k), 1)).astype(F32)
    rest = jnp.concatenate([gram, eye], axis=1)
    wide = rest.shape[1]
    ids = lax.broadcasted_iota(jnp.int32, (block, wide), 0)
    done = []
    for j in range(0, k, block):
        panel = rest[:block]
        diag = [jnp.broadcast_to(panel[:, j + i : j + i + 1], (block, wide)) for i in range(block)]
        scale = jnp.zeros((block, wide), F32)
        for i in range(block):
            pivot = diag[i][i : i + 1, :]
            scale = jnp.where(ids == i, lax.rsqrt(pivot), scale)
            if i + 1 < block:
                factor = jnp.where(ids > i, diag[i] * (1.0 / pivot), 0.0)
                panel = panel - factor * panel[i : i + 1, :]
                for m in range(i + 1, block):
                    diag[m] = diag[m] - factor * diag[m][i : i + 1, :]
        panel = panel * scale
        done.append(panel)
        if j + block < k:
            update = dot(panel[:, :k], panel, TN, HIGH)
            rest = rest[block:] - update[j + block :]
    return jnp.concatenate(done, axis=0)


def solve(factor, right):
    return dot(factor, jnp.concatenate([jnp.zeros_like(right), right], axis=0), NN, HIGH)


def added(refs):
    total = refs[0][...]
    for r in refs[1:]:
        total = total + r[...]
    return total


def basis_kernel(parts, *refs):
    grams, pieces, out = refs[:parts], refs[parts : 2 * parts], refs[-1]
    out[...] = solve(lower_inverse(added(grams)), added(pieces)).astype(BF)


def final_kernel(parts, scale, *refs):
    grams, pieces = refs[:parts], refs[parts : 2 * parts]
    total, basis_ref, load_ref = refs[2 * parts :]
    factor = lower_inverse(added(grams))
    load_ref[...] = solve(factor, added(pieces))
    basis_ref[...] = (solve(factor, total[...]) * scale).astype(BF)


def stages_of(n):
    stages = []
    step = 1
    while step < n:
        count = min(4, n // step)
        stages.append((step, count))
        step *= count
    return stages


def hop(value, distance, n):
    return lax.ppermute(value, "cell", [(i, i ^ distance) for i in range(n)])


def reduce_both(y, gram, n):
    stages = stages_of(n)
    for at, (step, count) in enumerate(stages):
        left = y.shape[0] // count
        y = y.reshape((left, count) + y.shape[1:])
        pieces = [y[:, 0]] + [hop(y[:, d], d * step, n) for d in range(1, count)]
        grams = [gram] + [hop(gram, d * step, n) for d in range(1, count)]
        if at + 1 < len(stages):
            y, gram = sum(pieces[1:], pieces[0]), sum(grams[1:], grams[0])
    return grams, [p[0] for p in pieces]


def gather(piece, n):
    whole = piece[None]
    for step, count in reversed(stages_of(n)):
        parts = [whole] + [hop(whole, d * step, n) for d in range(1, count)]
        whole = jnp.stack(parts, axis=1).reshape((-1,) + piece.shape)
    return whole


def local(tiles, tile_row, tile_col, tile_count, start_basis):
    n = lax.axis_size("cell")
    me = lax.axis_index("cell").astype(jnp.int32)
    slots, tile = tiles.shape[1], tiles.shape[-1]
    k, genes = start_basis.shape
    cells = ROW_BLOCKS * tile
    wide = genes // n
    aligned = wide % 128 == 0
    me_ref = me.reshape(1)

    x, half = pl.pallas_call(
        dense_kernel,
        out_shape=(jax.ShapeDtypeStruct((cells, genes), BF), jax.ShapeDtypeStruct((k, cells), F32)),
        in_specs=[SMEM, SMEM, SMEM, ANY, VMEM],
        out_specs=(VMEM, VMEM),
        scratch_shapes=[pltpu.SMEM((ROW_BLOCKS * (genes // tile),), jnp.int32), pltpu.SemaphoreType.DMA((slots,))],
        name="dense",
    )(tile_row, tile_col, tile_count, tiles[0], start_basis)

    def share(half, keep):
        other = lax.ppermute(half, "gene", [(0, 1), (1, 0)])
        y_shape = (n, k, wide) if aligned else (k, genes)
        shapes = [jax.ShapeDtypeStruct(y_shape, F32), jax.ShapeDtypeStruct((k, k), F32)]
        if keep:
            shapes.append(jax.ShapeDtypeStruct((k, cells), F32))
        y, gram, *total = pl.pallas_call(
            share_kernel,
            out_shape=tuple(shapes),
            in_specs=[SMEM, VMEM, VMEM, VMEM],
            out_specs=(VMEM,) * len(shapes),
            name="share",
        )(me_ref, half, other, x)
        if not aligned:
            y = jnp.transpose(y.reshape(k, n, wide), (1, 0, 2))[jnp.arange(n) ^ me]
        grams, pieces = reduce_both(y, gram, n)
        return grams, pieces, total

    grams, pieces, _ = share(half, False)
    piece = pl.pallas_call(
        functools.partial(basis_kernel, len(grams)),
        out_shape=jax.ShapeDtypeStruct((k, wide), BF),
        in_specs=[VMEM] * (2 * len(grams)),
        out_specs=VMEM,
        name="basis",
    )(*grams, *pieces)
    whole = gather(piece, n)[jnp.arange(n) ^ me]
    basis = jnp.transpose(whole, (1, 0, 2)).reshape(k, genes)
    half = pl.pallas_call(
        scores_kernel,
        out_shape=jax.ShapeDtypeStruct((k, cells), F32),
        in_specs=[VMEM, VMEM],
        out_specs=VMEM,
        name="scores",
    )(basis, x)
    grams, pieces, (total,) = share(half, True)
    scale = float(n * cells) ** 0.5
    return pl.pallas_call(
        functools.partial(final_kernel, len(grams), scale),
        out_shape=(jax.ShapeDtypeStruct((k, cells), BF), jax.ShapeDtypeStruct((k, wide), F32)),
        in_specs=[VMEM] * (2 * len(grams) + 1),
        out_specs=(VMEM, VMEM),
        name="final",
    )(*grams, *pieces, total)


def solution(mesh):
    return jax.shard_map(
        local,
        mesh=mesh,
        in_specs=(
            P("gene", "cell", None, None),
            P("gene", "cell"),
            P("gene", "cell"),
            P("gene", "cell"),
            P(None, "gene"),
        ),
        out_specs=(P(None, "cell"), P(None, ("gene", "cell"))),
        check_vma=False,
    )
```

```python
import functools

import jax
import jax.numpy as jnp
from jax import lax
from jax.experimental import pallas as pl
from jax.experimental.pallas import tpu as pltpu
from jax.sharding import PartitionSpec as P

ROW_BLOCKS = 8
BF = jnp.bfloat16
F32 = jnp.float32
HIGH = lax.Precision.HIGHEST
NT = (((1,), (1,)), ((), ()))
TN = (((0,), (0,)), ((), ()))
NN = (((1,), (0,)), ((), ()))
VMEM = pl.BlockSpec(memory_space=pltpu.VMEM)
SMEM = pl.BlockSpec(memory_space=pltpu.SMEM)
ANY = pl.BlockSpec(memory_space=pl.ANY)


def dot(a, b, dims, precision=None):
    return lax.dot_general(a, b, dims, precision=precision, preferred_element_type=F32)


def dense_kernel(row, col, count, tiles, basis, x_ref, s_ref, held, sems):
    tile = tiles.shape[-1]
    rows = x_ref.shape[0] // tile
    cols = x_ref.shape[1] // tile

    def place(r, c):
        return x_ref.at[pl.ds(pl.multiple_of(r * tile, tile), tile), pl.ds(pl.multiple_of(c * tile, tile), tile)]

    def copy(s):
        return pltpu.make_async_copy(tiles.at[s], place(row[0, s], col[0, s]), sems.at[s])

    for i in range(rows * cols):
        held[i] = 0
    live = count[0, 0]

    def start(s, _):
        copy(s).start()
        held[row[0, s] * cols + col[0, s]] = 1
        return 0

    lax.fori_loop(0, live, start, 0)

    def clear(i, _):
        @pl.when(held[i] == 0)
        def _():
            spot = place(i // cols, lax.rem(i, cols))
            spot[...] = jnp.zeros((tile, tile), BF)

        return 0

    lax.fori_loop(0, rows * cols, clear, 0)

    def finish(s, _):
        copy(s).wait()
        return 0

    lax.fori_loop(0, live, finish, 0)
    s_ref[...] = dot(basis[...], x_ref[...], NT)


def scores_kernel(pieces, x, s_ref):
    s_ref[...] = dot(pieces[...], x[...], NT)


def scores_parts_kernel(count, me, *refs):
    parts, (x, s_ref, held) = refs[:count], refs[count:]
    _, _, wide = parts[0].shape
    for d in range(count):
        for a in range(parts[d].shape[0]):
            q = jnp.bitwise_xor(me[0], a * count + d)
            held[:, pl.ds(pl.multiple_of(q * wide, wide), wide)] = parts[d][a]
    s_ref[...] = dot(held[...], x[...], NT)


def product(total, x):
    k = total.shape[0]
    high = total.astype(BF)
    low = (total - high.astype(F32)).astype(BF)
    both = jnp.concatenate([high, low], axis=0)
    y = dot(both, x, NN)
    g = dot(both, high, NT)
    h = dot(both, low, NT)
    return y[:k] + y[k:], (g[:k] + (g[k:] + h[:k])) + h[k:]


def share_kernel(me, own, other, x, y_ref, gram_ref, total_ref=None):
    total = own[...] + other[...]
    if total_ref is not None:
        total_ref[...] = total
    y_ref[...], gram_ref[...] = product(total, x[...])


def packed_kernel(n, count, keep, me, own, other, x, *refs):
    outs, y_ref = refs[:count], refs[-1]
    total = own[...] + other[...]
    if keep:
        refs[count][...] = total
    y, gram = product(total, x[...])
    k = gram.shape[0]
    wide = y_ref.shape[2]
    for q in range(n):
        y_ref[q] = y[:, q * wide : (q + 1) * wide]
    eye = (lax.broadcasted_iota(jnp.int32, (k, k), 0) == lax.broadcasted_iota(jnp.int32, (k, k), 1)).astype(F32)
    tail = jnp.concatenate([gram, eye * (1.0 / n)], axis=1)
    left = n // count
    for d in range(count):
        for a in range(left):
            outs[d][a] = y_ref[jnp.bitwise_xor(me[0], a * count + d)]
        outs[d][left] = tail


def mid_kernel(parts, count, *refs):
    sources, outs = refs[:parts], refs[parts:]
    left = (sources[0].shape[0] - 1) // count
    tail = added([s.at[left * count] for s in sources])
    for d in range(count):
        for a in range(left):
            outs[d][a] = added([s.at[a * count + d] for s in sources])
        outs[d][left] = tail


def with_identity(gram):
    k = gram.shape[0]
    eye = (lax.broadcasted_iota(jnp.int32, (k, k), 0) == lax.broadcasted_iota(jnp.int32, (k, k), 1)).astype(F32)
    return jnp.concatenate([gram, eye], axis=1)


def lower_inverse(rest, block=8):
    k = rest.shape[0]
    wide = rest.shape[1]
    ids = lax.broadcasted_iota(jnp.int32, (block, wide), 0)
    done = []
    for j in range(0, k, block):
        panel = rest[:block]
        diag = [jnp.broadcast_to(panel[:, j + i : j + i + 1], (block, wide)) for i in range(block)]
        scale = jnp.zeros((block, wide), F32)
        for i in range(block):
            pivot = diag[i][i : i + 1, :]
            scale = jnp.where(ids == i, lax.rsqrt(pivot), scale)
            if i + 1 < block:
                factor = jnp.where(ids > i, diag[i] * (1.0 / pivot), 0.0)
                panel = panel - factor * panel[i : i + 1, :]
                for m in range(i + 1, block):
                    diag[m] = diag[m] - factor * diag[m][i : i + 1, :]
        panel = panel * scale
        done.append(panel)
        if j + block < k:
            update = dot(panel[:, :k], panel, TN, HIGH)
            rest = rest[block:] - update[j + block :]
    return jnp.concatenate(done, axis=0)


def solve(factor, right):
    return dot(factor, jnp.concatenate([jnp.zeros_like(right), right], axis=0), NN, HIGH)


def added(refs):
    total = refs[0][...]
    for r in refs[1:]:
        total = total + r[...]
    return total


def gathered(parts, packed, refs):
    if packed:
        return added([r.at[1] for r in refs[:parts]]), added([r.at[0] for r in refs[:parts]]), refs[parts:]
    return with_identity(added(refs[:parts])), added(refs[parts : 2 * parts]), refs[2 * parts :]


def basis_kernel(parts, packed, *refs):
    gram, piece, (out,) = gathered(parts, packed, refs)
    out[...] = solve(lower_inverse(gram), piece).astype(BF)


def final_kernel(parts, packed, scale, *refs):
    gram, piece, (total, basis_ref, load_ref) = gathered(parts, packed, refs)
    factor = lower_inverse(gram)
    load_ref[...] = solve(factor, piece)
    basis_ref[...] = (solve(factor, total[...]) * scale).astype(BF)


def stages_of(n):
    stages = []
    step = 1
    while step < n:
        count = min(4, n // step)
        stages.append((step, count))
        step *= count
    return stages


def hop(value, distance, n):
    return lax.ppermute(value, "cell", [(i, i ^ distance) for i in range(n)])


def reduce_both(y, gram, n):
    stages = stages_of(n)
    for at, (step, count) in enumerate(stages):
        left = y.shape[0] // count
        y = y.reshape((left, count) + y.shape[1:])
        pieces = [y[:, 0]] + [hop(y[:, d], d * step, n) for d in range(1, count)]
        grams = [gram] + [hop(gram, d * step, n) for d in range(1, count)]
        if at + 1 < len(stages):
            y, gram = sum(pieces[1:], pieces[0]), sum(grams[1:], grams[0])
    return grams, [p[0] for p in pieces]


def gather(piece, n):
    parts = [piece[None]]
    for step, count in reversed(stages_of(n)):
        whole = jnp.stack(parts, axis=1).reshape((-1,) + piece.shape)
        parts = [whole] + [hop(whole, d * step, n) for d in range(1, count)]
    return parts


def local(tiles, tile_row, tile_col, tile_count, start_basis):
    n = lax.axis_size("cell")
    me = lax.axis_index("cell").astype(jnp.int32)
    slots, tile = tiles.shape[1], tiles.shape[-1]
    k, genes = start_basis.shape
    cells = ROW_BLOCKS * tile
    wide = genes // n
    me_ref = me.reshape(1)

    x, half = pl.pallas_call(
        dense_kernel,
        out_shape=(jax.ShapeDtypeStruct((cells, genes), BF), jax.ShapeDtypeStruct((k, cells), F32)),
        in_specs=[SMEM, SMEM, SMEM, ANY, VMEM],
        out_specs=(VMEM, VMEM),
        scratch_shapes=[pltpu.SMEM((ROW_BLOCKS * (genes // tile),), jnp.int32), pltpu.SemaphoreType.DMA((slots,))],
        name="dense",
    )(tile_row, tile_col, tile_count, tiles[0], start_basis)

    stages = stages_of(n)
    packed = wide == tile and 2 * k == wide

    def share(half, keep):
        other = lax.ppermute(half, "gene", [(0, 1), (1, 0)])
        kept = [jax.ShapeDtypeStruct((k, cells), F32)] * keep
        if not packed:
            shapes = [jax.ShapeDtypeStruct((k, genes), F32), jax.ShapeDtypeStruct((k, k), F32)] + kept
            y, gram, *total = pl.pallas_call(
                share_kernel,
                out_shape=tuple(shapes),
                in_specs=[SMEM, VMEM, VMEM, VMEM],
                out_specs=(VMEM,) * len(shapes),
                name="share",
            )(me_ref, half, other, x)
            y = jnp.transpose(y.reshape(k, n, wide), (1, 0, 2))[jnp.arange(n) ^ me]
            grams, pieces = reduce_both(y, gram, n)
            return grams + pieces, total
        left = n
        for at, (step, count) in enumerate(stages):
            left = left // count
            shapes = [jax.ShapeDtypeStruct((left + 1, k, wide), F32)] * count
            if at == 0:
                outs = pl.pallas_call(
                    functools.partial(packed_kernel, n, count, keep),
                    out_shape=tuple(shapes + kept),
                    in_specs=[SMEM, VMEM, VMEM, VMEM],
                    out_specs=(VMEM,) * (count + keep),
                    scratch_shapes=[pltpu.VMEM((n, k, wide), F32)],
                    name="share",
                )(me_ref, half, other, x)
                total = outs[count:]
            else:
                outs = pl.pallas_call(
                    functools.partial(mid_kernel, len(parts), count),
                    out_shape=tuple(shapes),
                    in_specs=[VMEM] * len(parts),
                    out_specs=(VMEM,) * count,
                    name="mid",
                )(*parts)
            parts = [outs[0]] + [hop(outs[d], d * step, n) for d in range(1, count)]
        return parts, total

    parts, _ = share(half, 0)
    last = stages[-1][1]
    piece = pl.pallas_call(
        functools.partial(basis_kernel, last, packed),
        out_shape=jax.ShapeDtypeStruct((k, wide), BF),
        in_specs=[VMEM] * len(parts),
        out_specs=VMEM,
        name="basis",
    )(*parts)
    parts = gather(piece, n)
    half_shape = jax.ShapeDtypeStruct((k, cells), F32)
    if packed:
        half = pl.pallas_call(
            functools.partial(scores_parts_kernel, len(parts)),
            out_shape=half_shape,
            in_specs=[SMEM] + [VMEM] * (len(parts) + 1),
            out_specs=VMEM,
            scratch_shapes=[pltpu.VMEM((k, genes), BF)],
            name="scores",
        )(me_ref, *parts, x)
    else:
        whole = jnp.stack(parts, axis=1).reshape(n, k, wide)[jnp.arange(n) ^ me]
        basis = jnp.transpose(whole, (1, 0, 2)).reshape(k, genes)
        half = pl.pallas_call(
            scores_kernel, out_shape=half_shape, in_specs=[VMEM, VMEM], out_specs=VMEM, name="scores"
        )(basis, x)
    parts, (total,) = share(half, 1)
    scale = float(n * cells) ** 0.5
    return pl.pallas_call(
        functools.partial(final_kernel, last, packed, scale),
        out_shape=(jax.ShapeDtypeStruct((k, cells), BF), jax.ShapeDtypeStruct((k, wide), F32)),
        in_specs=[VMEM] * (len(parts) + 1),
        out_specs=(VMEM, VMEM),
        name="final",
    )(*parts, total)


def solution(mesh):
    return jax.shard_map(
        local,
        mesh=mesh,
        in_specs=(
            P("gene", "cell", None, None),
            P("gene", "cell"),
            P("gene", "cell"),
            P("gene", "cell"),
            P(None, "gene"),
        ),
        out_specs=(P(None, "cell"), P(None, ("gene", "cell"))),
        check_vma=False,
    )
```

```python
import functools

import jax
import jax.numpy as jnp
from jax import lax
from jax.experimental import pallas as pl
from jax.experimental.pallas import tpu as pltpu
from jax.sharding import PartitionSpec as P

ROW_BLOCKS = 8
BF = jnp.bfloat16
F32 = jnp.float32
HIGH = lax.Precision.HIGHEST
NT = (((1,), (1,)), ((), ()))
TN = (((0,), (0,)), ((), ()))
NN = (((1,), (0,)), ((), ()))
VMEM = pl.BlockSpec(memory_space=pltpu.VMEM)
SMEM = pl.BlockSpec(memory_space=pltpu.SMEM)
ANY = pl.BlockSpec(memory_space=pl.ANY)


PARAMS = pltpu.CompilerParams(vmem_limit_bytes=24 * 1024 * 1024)


def dot(a, b, dims, precision=None):
    return lax.dot_general(a, b, dims, precision=precision, preferred_element_type=F32)


def dense_kernel(row, col, count, tiles, basis, x_ref, s_ref, held, sems):
    tile = tiles.shape[-1]
    rows = x_ref.shape[0] // tile
    cols = x_ref.shape[1] // tile

    def place(r, c):
        return x_ref.at[pl.ds(pl.multiple_of(r * tile, tile), tile), pl.ds(pl.multiple_of(c * tile, tile), tile)]

    def copy(s):
        return pltpu.make_async_copy(tiles.at[s], place(row[0, s], col[0, s]), sems.at[s])

    for i in range(rows * cols):
        held[i] = 0
    live = count[0, 0]

    def start(s, _):
        copy(s).start()
        held[row[0, s] * cols + col[0, s]] = 1
        return 0

    lax.fori_loop(0, live, start, 0)

    def clear(i, _):
        @pl.when(held[i] == 0)
        def _():
            spot = place(i // cols, lax.rem(i, cols))
            spot[...] = jnp.zeros((tile, tile), BF)

        return 0

    lax.fori_loop(0, rows * cols, clear, 0)

    def finish(s, _):
        copy(s).wait()
        return 0

    lax.fori_loop(0, live, finish, 0)
    s_ref[...] = dot(basis[...], x_ref[...], NT)


def scores_kernel(pieces, x, s_ref):
    s_ref[...] = dot(pieces[...], x[...], NT)


def scores_parts_kernel(count, me, *refs):
    parts, (x, s_ref, held) = refs[:count], refs[count:]
    _, _, wide = parts[0].shape
    for d in range(count):
        for a in range(parts[d].shape[0]):
            q = jnp.bitwise_xor(me[0], a * count + d)
            held[:, pl.ds(pl.multiple_of(q * wide, wide), wide)] = parts[d][a]
    s_ref[...] = dot(held[...], x[...], NT)


def product(total, x):
    k = total.shape[0]
    high = total.astype(BF)
    low = (total - high.astype(F32)).astype(BF)
    both = jnp.concatenate([high, low], axis=0)
    y = dot(both, x, NN)
    g = dot(both, high, NT)
    h = dot(both, low, NT)
    return y[:k] + y[k:], (g[:k] + (g[k:] + h[:k])) + h[k:]


def share_kernel(me, own, other, x, y_ref, gram_ref, total_ref=None):
    total = own[...] + other[...]
    if total_ref is not None:
        total_ref[...] = total
    y_ref[...], gram_ref[...] = product(total, x[...])


def packed_kernel(n, count, keep, me, own, other, x, *refs):
    outs, y_ref = refs[:count], refs[-1]
    total = own[...] + other[...]
    if keep:
        refs[count][...] = total
    y, gram = product(total, x[...])
    k = gram.shape[0]
    wide = y_ref.shape[2]
    for q in range(n):
        y_ref[q] = y[:, q * wide : (q + 1) * wide]
    eye = (lax.broadcasted_iota(jnp.int32, (k, k), 0) == lax.broadcasted_iota(jnp.int32, (k, k), 1)).astype(F32)
    tail = jnp.concatenate([gram, eye * (1.0 / n)], axis=1)
    left = n // count
    for d in range(count):
        for a in range(left):
            outs[d][a] = y_ref[jnp.bitwise_xor(me[0], a * count + d)]
        outs[d][left] = tail


def mid_kernel(parts, count, *refs):
    sources, outs = refs[:parts], refs[parts:]
    left = (sources[0].shape[0] - 1) // count
    tail = added([s.at[left * count] for s in sources])
    for d in range(count):
        for a in range(left):
            outs[d][a] = added([s.at[a * count + d] for s in sources])
        outs[d][left] = tail


def with_identity(gram):
    k = gram.shape[0]
    eye = (lax.broadcasted_iota(jnp.int32, (k, k), 0) == lax.broadcasted_iota(jnp.int32, (k, k), 1)).astype(F32)
    return jnp.concatenate([gram, eye], axis=1)


def lower_inverse(rest, block=8):
    k = rest.shape[0]
    wide = rest.shape[1]
    ids = lax.broadcasted_iota(jnp.int32, (block, wide), 0)
    done = []
    for j in range(0, k, block):
        panel = rest[:block]
        diag = [jnp.broadcast_to(panel[:, j + i : j + i + 1], (block, wide)) for i in range(block)]
        scale = jnp.zeros((block, wide), F32)
        for i in range(block):
            pivot = diag[i][i : i + 1, :]
            scale = jnp.where(ids == i, lax.rsqrt(pivot), scale)
            if i + 1 < block:
                factor = jnp.where(ids > i, diag[i] * (1.0 / pivot), 0.0)
                panel = panel - factor * panel[i : i + 1, :]
                for m in range(i + 1, block):
                    diag[m] = diag[m] - factor * diag[m][i : i + 1, :]
        panel = panel * scale
        done.append(panel)
        if j + block < k:
            update = dot(panel[:, :k], panel, TN, HIGH)
            rest = rest[block:] - update[j + block :]
    return jnp.concatenate(done, axis=0)


def solve(factor, right):
    return dot(factor, jnp.concatenate([jnp.zeros_like(right), right], axis=0), NN, HIGH)


def added(refs):
    total = refs[0][...]
    for r in refs[1:]:
        total = total + r[...]
    return total


def gathered(parts, packed, refs):
    if packed:
        return added([r.at[1] for r in refs[:parts]]), added([r.at[0] for r in refs[:parts]]), refs[parts:]
    return with_identity(added(refs[:parts])), added(refs[parts : 2 * parts]), refs[2 * parts :]


def basis_kernel(parts, packed, *refs):
    gram, piece, (out,) = gathered(parts, packed, refs)
    out[...] = solve(lower_inverse(gram), piece).astype(BF)


def final_kernel(parts, packed, scale, *refs):
    gram, piece, (total, basis_ref, load_ref) = gathered(parts, packed, refs)
    factor = lower_inverse(gram)
    load_ref[...] = solve(factor, piece)
    basis_ref[...] = (solve(factor, total[...]) * scale).astype(BF)


def stages_of(n):
    stages = []
    step = 1
    while step < n:
        count = min(4, n // step)
        stages.append((step, count))
        step *= count
    return stages


def hop(value, distance, n):
    return lax.ppermute(value, "cell", [(i, i ^ distance) for i in range(n)])


def reduce_both(y, gram, n):
    stages = stages_of(n)
    for at, (step, count) in enumerate(stages):
        left = y.shape[0] // count
        y = y.reshape((left, count) + y.shape[1:])
        pieces = [y[:, 0]] + [hop(y[:, d], d * step, n) for d in range(1, count)]
        grams = [gram] + [hop(gram, d * step, n) for d in range(1, count)]
        if at + 1 < len(stages):
            y, gram = sum(pieces[1:], pieces[0]), sum(grams[1:], grams[0])
    return grams, [p[0] for p in pieces]


def gather(piece, n):
    parts = [piece[None]]
    for step, count in reversed(stages_of(n)):
        whole = jnp.stack(parts, axis=1).reshape((-1,) + piece.shape)
        parts = [whole] + [hop(whole, d * step, n) for d in range(1, count)]
    return parts


def local(tiles, tile_row, tile_col, tile_count, start_basis):
    n = lax.axis_size("cell")
    me = lax.axis_index("cell").astype(jnp.int32)
    slots, tile = tiles.shape[1], tiles.shape[-1]
    k, genes = start_basis.shape
    cells = ROW_BLOCKS * tile
    wide = genes // n
    me_ref = me.reshape(1)

    x, half = pl.pallas_call(
        dense_kernel,
        out_shape=(pltpu.VMEM((cells, genes), BF), jax.ShapeDtypeStruct((k, cells), F32)),
        in_specs=[SMEM, SMEM, SMEM, ANY, VMEM],
        out_specs=(VMEM, VMEM),
        scratch_shapes=[pltpu.SMEM((ROW_BLOCKS * (genes // tile),), jnp.int32), pltpu.SemaphoreType.DMA((slots,))],
        compiler_params=PARAMS,
        name="dense",
    )(tile_row, tile_col, tile_count, tiles[0], start_basis)

    stages = stages_of(n)
    packed = wide == tile and 2 * k == wide

    def share(half, keep):
        other = lax.ppermute(half, "gene", [(0, 1), (1, 0)])
        kept = [jax.ShapeDtypeStruct((k, cells), F32)] * keep
        if not packed:
            shapes = [jax.ShapeDtypeStruct((k, genes), F32), jax.ShapeDtypeStruct((k, k), F32)] + kept
            y, gram, *total = pl.pallas_call(
                share_kernel,
                out_shape=tuple(shapes),
                in_specs=[SMEM, VMEM, VMEM, VMEM],
                out_specs=(VMEM,) * len(shapes),
                compiler_params=PARAMS,
                name="share",
            )(me_ref, half, other, x)
            y = jnp.transpose(y.reshape(k, n, wide), (1, 0, 2))[jnp.arange(n) ^ me]
            grams, pieces = reduce_both(y, gram, n)
            return grams + pieces, total
        left = n
        for at, (step, count) in enumerate(stages):
            left = left // count
            shapes = [jax.ShapeDtypeStruct((left + 1, k, wide), F32)] * count
            if at == 0:
                outs = pl.pallas_call(
                    functools.partial(packed_kernel, n, count, keep),
                    out_shape=tuple(shapes + kept),
                    in_specs=[SMEM, VMEM, VMEM, VMEM],
                    out_specs=(VMEM,) * (count + keep),
                    scratch_shapes=[pltpu.VMEM((n, k, wide), F32)],
                    compiler_params=PARAMS,
                    name="share",
                )(me_ref, half, other, x)
                total = outs[count:]
            else:
                outs = pl.pallas_call(
                    functools.partial(mid_kernel, len(parts), count),
                    out_shape=tuple(shapes),
                    in_specs=[VMEM] * len(parts),
                    out_specs=(VMEM,) * count,
                    compiler_params=PARAMS,
                    name="mid",
                )(*parts)
            parts = [outs[0]] + [hop(outs[d], d * step, n) for d in range(1, count)]
        return parts, total

    parts, _ = share(half, 0)
    last = stages[-1][1]
    piece = pl.pallas_call(
        functools.partial(basis_kernel, last, packed),
        out_shape=jax.ShapeDtypeStruct((k, wide), BF),
        in_specs=[VMEM] * len(parts),
        out_specs=VMEM,
        compiler_params=PARAMS,
        name="basis",
    )(*parts)
    parts = gather(piece, n)
    half_shape = jax.ShapeDtypeStruct((k, cells), F32)
    if packed:
        half = pl.pallas_call(
            functools.partial(scores_parts_kernel, len(parts)),
            out_shape=half_shape,
            in_specs=[SMEM] + [VMEM] * (len(parts) + 1),
            out_specs=VMEM,
            scratch_shapes=[pltpu.VMEM((k, genes), BF)],
            compiler_params=PARAMS,
            name="scores",
        )(me_ref, *parts, x)
    else:
        whole = jnp.stack(parts, axis=1).reshape(n, k, wide)[jnp.arange(n) ^ me]
        basis = jnp.transpose(whole, (1, 0, 2)).reshape(k, genes)
        half = pl.pallas_call(
            scores_kernel, out_shape=half_shape, in_specs=[VMEM, VMEM], out_specs=VMEM, compiler_params=PARAMS, name="scores"
        )(basis, x)
    parts, (total,) = share(half, 1)
    scale = float(n * cells) ** 0.5
    return pl.pallas_call(
        functools.partial(final_kernel, last, packed, scale),
        out_shape=(jax.ShapeDtypeStruct((k, cells), BF), jax.ShapeDtypeStruct((k, wide), F32)),
        in_specs=[VMEM] * (len(parts) + 1),
        out_specs=(VMEM, VMEM),
        compiler_params=PARAMS,
        name="final",
    )(*parts, total)


def solution(mesh):
    return jax.shard_map(
        local,
        mesh=mesh,
        in_specs=(
            P("gene", "cell", None, None),
            P("gene", "cell"),
            P("gene", "cell"),
            P("gene", "cell"),
            P(None, "gene"),
        ),
        out_specs=(P(None, "cell"), P(None, ("gene", "cell"))),
        check_vma=False,
    )
```

```python
import functools

import jax
import jax.numpy as jnp
from jax import lax
from jax.experimental import pallas as pl
from jax.experimental.pallas import tpu as pltpu
from jax.sharding import PartitionSpec as P

ROW_BLOCKS = 8
BF = jnp.bfloat16
F32 = jnp.float32
HIGH = lax.Precision.HIGHEST
NT = (((1,), (1,)), ((), ()))
TN = (((0,), (0,)), ((), ()))
NN = (((1,), (0,)), ((), ()))
VMEM = pl.BlockSpec(memory_space=pltpu.VMEM)
SMEM = pl.BlockSpec(memory_space=pltpu.SMEM)
ANY = pl.BlockSpec(memory_space=pl.ANY)


PARAMS = pltpu.CompilerParams(vmem_limit_bytes=24 * 1024 * 1024)


def dot(a, b, dims, precision=None):
    return lax.dot_general(a, b, dims, precision=precision, preferred_element_type=F32)


def dense_kernel(row, col, count, tiles, basis, x_ref, s_ref, sems):
    tile = tiles.shape[-1]
    slots = tiles.shape[0]
    x_ref[...] = jnp.zeros(x_ref.shape, BF)

    def copy(s):
        r, c = pl.multiple_of(row[0, s] * tile, tile), pl.multiple_of(col[0, s] * tile, tile)
        return pltpu.make_async_copy(tiles.at[s], x_ref.at[pl.ds(r, tile), pl.ds(c, tile)], sems.at[s])

    for s in range(slots):
        @pl.when(s < count[0, 0])
        def _():
            copy(s).start()

    for s in range(slots):
        @pl.when(s < count[0, 0])
        def _():
            copy(s).wait()

    s_ref[...] = dot(basis[...], x_ref[...], NT)


def scores_kernel(pieces, x, s_ref):
    s_ref[...] = dot(pieces[...], x[...], NT)


def scores_parts_kernel(count, me, *refs):
    parts, (x, s_ref, held) = refs[:count], refs[count:]
    _, _, wide = parts[0].shape
    for d in range(count):
        for a in range(parts[d].shape[0]):
            q = jnp.bitwise_xor(me[0], a * count + d)
            held[:, pl.ds(pl.multiple_of(q * wide, wide), wide)] = parts[d][a]
    s_ref[...] = dot(held[...], x[...], NT)


def product(total, x):
    k = total.shape[0]
    high = total.astype(BF)
    low = (total - high.astype(F32)).astype(BF)
    both = jnp.concatenate([high, low], axis=0)
    y = dot(both, x, NN)
    g = dot(both, high, NT)
    h = dot(both, low, NT)
    return y[:k] + y[k:], (g[:k] + (g[k:] + h[:k])) + h[k:]


def share_kernel(me, own, other, x, y_ref, gram_ref, total_ref=None):
    total = own[...] + other[...]
    if total_ref is not None:
        total_ref[...] = total
    y_ref[...], gram_ref[...] = product(total, x[...])


def packed_kernel(n, count, keep, me, own, other, x, *refs):
    outs, y_ref = refs[:count], refs[-1]
    total = own[...] + other[...]
    if keep:
        refs[count][...] = total
    y, gram = product(total, x[...])
    k = gram.shape[0]
    wide = y_ref.shape[2]
    for q in range(n):
        y_ref[q] = y[:, q * wide : (q + 1) * wide]
    eye = (lax.broadcasted_iota(jnp.int32, (k, k), 0) == lax.broadcasted_iota(jnp.int32, (k, k), 1)).astype(F32)
    tail = jnp.concatenate([gram, eye * (1.0 / n)], axis=1)
    left = n // count
    for d in range(count):
        for a in range(left):
            outs[d][a] = y_ref[jnp.bitwise_xor(me[0], a * count + d)]
        outs[d][left] = tail


def mid_kernel(parts, count, *refs):
    sources, outs = refs[:parts], refs[parts:]
    left = (sources[0].shape[0] - 1) // count
    tail = added([s.at[left * count] for s in sources])
    for d in range(count):
        for a in range(left):
            outs[d][a] = added([s.at[a * count + d] for s in sources])
        outs[d][left] = tail


def with_identity(gram):
    k = gram.shape[0]
    eye = (lax.broadcasted_iota(jnp.int32, (k, k), 0) == lax.broadcasted_iota(jnp.int32, (k, k), 1)).astype(F32)
    return jnp.concatenate([gram, eye], axis=1)


def lower_inverse(rest, block=8):
    k = rest.shape[0]
    wide = rest.shape[1]
    ids = lax.broadcasted_iota(jnp.int32, (block, wide), 0)
    done = []
    for j in range(0, k, block):
        panel = rest[:block]
        diag = [jnp.broadcast_to(panel[:, j + i : j + i + 1], (block, wide)) for i in range(block)]
        scale = jnp.zeros((block, wide), F32)
        for i in range(block):
            pivot = diag[i][i : i + 1, :]
            scale = jnp.where(ids == i, lax.rsqrt(pivot), scale)
            if i + 1 < block:
                factor = jnp.where(ids > i, diag[i] * (1.0 / pivot), 0.0)
                panel = panel - factor * panel[i : i + 1, :]
                for m in range(i + 1, block):
                    diag[m] = diag[m] - factor * diag[m][i : i + 1, :]
        panel = panel * scale
        done.append(panel)
        if j + block < k:
            update = dot(panel[:, :k], panel, TN, HIGH)
            rest = rest[block:] - update[j + block :]
    return jnp.concatenate(done, axis=0)


def solve(factor, right):
    return dot(factor, jnp.concatenate([jnp.zeros_like(right), right], axis=0), NN, HIGH)


def added(refs):
    total = refs[0][...]
    for r in refs[1:]:
        total = total + r[...]
    return total


def gathered(parts, packed, refs):
    if packed:
        return added([r.at[1] for r in refs[:parts]]), added([r.at[0] for r in refs[:parts]]), refs[parts:]
    return with_identity(added(refs[:parts])), added(refs[parts : 2 * parts]), refs[2 * parts :]


def basis_kernel(parts, packed, *refs):
    gram, piece, (out,) = gathered(parts, packed, refs)
    out[...] = solve(lower_inverse(gram), piece).astype(BF)


def final_kernel(parts, packed, scale, *refs):
    gram, piece, (total, basis_ref, load_ref) = gathered(parts, packed, refs)
    factor = lower_inverse(gram)
    load_ref[...] = solve(factor, piece)
    basis_ref[...] = (solve(factor, total[...]) * scale).astype(BF)


def stages_of(n):
    stages = []
    step = 1
    while step < n:
        count = min(4, n // step)
        stages.append((step, count))
        step *= count
    return stages


def hop(value, distance, n):
    return lax.ppermute(value, "cell", [(i, i ^ distance) for i in range(n)])


def reduce_both(y, gram, n):
    stages = stages_of(n)
    for at, (step, count) in enumerate(stages):
        left = y.shape[0] // count
        y = y.reshape((left, count) + y.shape[1:])
        pieces = [y[:, 0]] + [hop(y[:, d], d * step, n) for d in range(1, count)]
        grams = [gram] + [hop(gram, d * step, n) for d in range(1, count)]
        if at + 1 < len(stages):
            y, gram = sum(pieces[1:], pieces[0]), sum(grams[1:], grams[0])
    return grams, [p[0] for p in pieces]


def gather(piece, n):
    parts = [piece[None]]
    for step, count in reversed(stages_of(n)):
        whole = jnp.stack(parts, axis=1).reshape((-1,) + piece.shape)
        parts = [whole] + [hop(whole, d * step, n) for d in range(1, count)]
    return parts


def local(tiles, tile_row, tile_col, tile_count, start_basis):
    n = lax.axis_size("cell")
    me = lax.axis_index("cell").astype(jnp.int32)
    slots, tile = tiles.shape[1], tiles.shape[-1]
    k, genes = start_basis.shape
    cells = ROW_BLOCKS * tile
    wide = genes // n
    me_ref = me.reshape(1)

    x, half = pl.pallas_call(
        dense_kernel,
        out_shape=(pltpu.VMEM((cells, genes), BF), jax.ShapeDtypeStruct((k, cells), F32)),
        in_specs=[SMEM, SMEM, SMEM, ANY, VMEM],
        out_specs=(VMEM, VMEM),
        scratch_shapes=[pltpu.SemaphoreType.DMA((slots,))],
        compiler_params=PARAMS,
        name="dense",
    )(tile_row, tile_col, tile_count, pltpu.with_memory_space_constraint(tiles[0], pltpu.HBM), start_basis)
    x = pltpu.with_memory_space_constraint(x, pltpu.VMEM)

    stages = stages_of(n)
    packed = wide == tile and 2 * k == wide

    def share(half, keep):
        other = lax.ppermute(half, "gene", [(0, 1), (1, 0)])
        kept = [jax.ShapeDtypeStruct((k, cells), F32)] * keep
        if not packed:
            shapes = [jax.ShapeDtypeStruct((k, genes), F32), jax.ShapeDtypeStruct((k, k), F32)] + kept
            y, gram, *total = pl.pallas_call(
                share_kernel,
                out_shape=tuple(shapes),
                in_specs=[SMEM, VMEM, VMEM, VMEM],
                out_specs=(VMEM,) * len(shapes),
                compiler_params=PARAMS,
                name="share",
            )(me_ref, half, other, x)
            y = jnp.transpose(y.reshape(k, n, wide), (1, 0, 2))[jnp.arange(n) ^ me]
            grams, pieces = reduce_both(y, gram, n)
            return grams + pieces, total
        left = n
        for at, (step, count) in enumerate(stages):
            left = left // count
            shapes = [jax.ShapeDtypeStruct((left + 1, k, wide), F32)] * count
            if at == 0:
                outs = pl.pallas_call(
                    functools.partial(packed_kernel, n, count, keep),
                    out_shape=tuple(shapes + kept),
                    in_specs=[SMEM, VMEM, VMEM, VMEM],
                    out_specs=(VMEM,) * (count + keep),
                    scratch_shapes=[pltpu.VMEM((n, k, wide), F32)],
                    compiler_params=PARAMS,
                    name="share",
                )(me_ref, half, other, x)
                total = outs[count:]
            else:
                outs = pl.pallas_call(
                    functools.partial(mid_kernel, len(parts), count),
                    out_shape=tuple(shapes),
                    in_specs=[VMEM] * len(parts),
                    out_specs=(VMEM,) * count,
                    compiler_params=PARAMS,
                    name="mid",
                )(*parts)
            parts = [outs[0]] + [hop(outs[d], d * step, n) for d in range(1, count)]
        return parts, total

    parts, _ = share(half, 0)
    last = stages[-1][1]
    piece = pl.pallas_call(
        functools.partial(basis_kernel, last, packed),
        out_shape=jax.ShapeDtypeStruct((k, wide), BF),
        in_specs=[VMEM] * len(parts),
        out_specs=VMEM,
        compiler_params=PARAMS,
        name="basis",
    )(*parts)
    parts = gather(piece, n)
    half_shape = jax.ShapeDtypeStruct((k, cells), F32)
    if packed:
        half = pl.pallas_call(
            functools.partial(scores_parts_kernel, len(parts)),
            out_shape=half_shape,
            in_specs=[SMEM] + [VMEM] * (len(parts) + 1),
            out_specs=VMEM,
            scratch_shapes=[pltpu.VMEM((k, genes), BF)],
            compiler_params=PARAMS,
            name="scores",
        )(me_ref, *parts, x)
    else:
        whole = jnp.stack(parts, axis=1).reshape(n, k, wide)[jnp.arange(n) ^ me]
        basis = jnp.transpose(whole, (1, 0, 2)).reshape(k, genes)
        half = pl.pallas_call(
            scores_kernel, out_shape=half_shape, in_specs=[VMEM, VMEM], out_specs=VMEM, compiler_params=PARAMS, name="scores"
        )(basis, x)
    parts, (total,) = share(half, 1)
    scale = float(n * cells) ** 0.5
    return pl.pallas_call(
        functools.partial(final_kernel, last, packed, scale),
        out_shape=(jax.ShapeDtypeStruct((k, cells), BF), jax.ShapeDtypeStruct((k, wide), F32)),
        in_specs=[VMEM] * (len(parts) + 1),
        out_specs=(VMEM, VMEM),
        compiler_params=PARAMS,
        name="final",
    )(*parts, total)


def solution(mesh):
    return jax.shard_map(
        local,
        mesh=mesh,
        in_specs=(
            P("gene", "cell", None, None),
            P("gene", "cell"),
            P("gene", "cell"),
            P("gene", "cell"),
            P(None, "gene"),
        ),
        out_specs=(P(None, "cell"), P(None, ("gene", "cell"))),
        check_vma=False,
    )
```
